32 devices in a mesh: fsdp: 4 (over y, x), ctx: 4 (over z), tp: 2 (over core).
Axes of the slice: x: 2, y: 2, z: 4, core: 2. Of those that a mesh axis runs over, the one named last changes fastest.
Arguments:
- tokens: bfloat16 [8, 1024, 768], P('fsdp', 'ctx'), may hold values from -6 to 6
- lengths: int32 [8], P('fsdp'), may hold values from 256 to 1024, as said below
- cotangent: bfloat16 [8, 1024, 768], P('fsdp', 'ctx'), may hold values from -6 to 6
- ln1_gain: float32 [768], replicated, may hold values from 0.5 to 1.5
- ln1_bias: float32 [768], replicated, may hold values from -1.8 to 1.8
- qkv_weight: bfloat16 [768, 3, 768], P('fsdp', None, 'tp'), may hold values from -0.21875 to 0.21875
- conv_kernel: float32 [3, 3, 768], P(None, None, 'tp'), may hold values from -3.5 to 3.5
- conv_bias: float32 [3, 768], P(None, 'tp'), may hold values from -1.8 to 1.8
- out_weight: bfloat16 [768, 768], P('tp', 'fsdp'), may hold values from -1.75 to 1.75
- ln2_gain: float32 [768], replicated, may hold values from 0.5 to 1.5
- ln2_bias: float32 [768], replicated, may hold values from -1.8 to 1.8
- up_weight: bfloat16 [768, 3072], P('fsdp', 'tp'), may hold values from -0.21875 to 0.21875
- down_weight: bfloat16 [3072, 768], P('tp', 'fsdp'), may hold values from -0.109375 to 0.109375
Outputs:
- result: bfloat16 [8, 1024, 768], P('fsdp', 'ctx')
- input_grad: float32 [8, 1024, 768], P('fsdp', 'ctx')
- ln1_gain_grad: float32 [768], replicated
- ln1_bias_grad: float32 [768], replicated
- qkv_weight_grad: float32 [768, 3, 768], P('fsdp', None, 'tp')
- conv_kernel_grad: float32 [3, 3, 768], P(None, None, 'tp')
- conv_bias_grad: float32 [3, 768], P(None, 'tp')
- out_weight_grad: float32 [768, 768], P('tp', 'fsdp')
- ln2_gain_grad: float32 [768], replicated
- ln2_bias_grad: float32 [768], replicated
- up_weight_grad: float32 [768, 3072], P('fsdp', 'tp')
- down_weight_grad: float32 [3072, 768], P('tp', 'fsdp')
The draws below stay inside these ranges and needn't reach their ends.
Inputs may be any that keep to these rules, and one draw needn't show every extreme that they name: `lengths`: some slot holds 1024 tokens and some other slot 256.
All inputs are finite; a program needn't handle non-finite values.
Results may differ from the reference program's by a relative error of at most 0.014.
The reference program's roundings to bfloat16 on the way count: a program that leaves them out, or rounds other values in their place, can miss the bound.
Values may be sent and summed in bfloat16 or wider, within the bound.
A program may use at most 256 MiB of HBM per device.

```python
import jax
import jax.numpy as jnp
from jax import lax

D = 768
H = 12
HD = 64
FF = 3072
HH = 768
S = 1024
SLOTS = 8


def draw_lengths(key, part):
    drawn = jax.random.randint(jax.random.fold_in(key, 11), (SLOTS,), S // 4, S + 1)
    chosen = jax.random.permutation(jax.random.fold_in(key, 12), SLOTS)
    drawn = drawn.at[chosen[0]].set(S)
    drawn = drawn.at[chosen[1]].set(S // 4)
    return drawn.astype(jnp.int32)


def block_levels(key, shape, split, low, high):
    level = 1.0
    for axis_at, parts in split:
        heights = jax.random.uniform(jax.random.fold_in(jax.random.fold_in(key, 6), axis_at), (parts,), jnp.float32, low / len(split), high / len(split))
        level = level * jnp.repeat(jnp.exp(heights), shape[axis_at] // parts).reshape((-1,) + (1,) * (len(shape) - 1 - axis_at))
    return level


def normal_values(stream_key, shape, deviation, most, cuts=(), kind=jnp.bfloat16):
    array = deviation * jax.random.normal(stream_key, shape, jnp.float32)
    if cuts:
        array = array * block_levels(stream_key, shape, cuts, -0.22, 0.18)
    return jnp.clip(array, -most, most).astype(kind)


def setup_inputs(seed: int = 0) -> dict:
    keys = jax.random.split(jax.random.key(seed), 14)
    return {
        "tokens": normal_values(keys[0], (SLOTS, S, D), 1.0, 6.0, ((0, 4), (1, 4))),
        "lengths": draw_lengths(jax.random.fold_in(keys[13], 71), 0),
        "cotangent": normal_values(keys[2], (SLOTS, S, D), 1.0, 6.0, ((0, 4), (1, 4))),
        "ln1_gain": jnp.clip(1.0 + 0.1 * jax.random.normal(keys[3], (D,), jnp.float32), 0.5, 1.5),
        "ln1_bias": normal_values(keys[4], (D,), 0.3, 1.8, (), jnp.float32),
        "qkv_weight": normal_values(keys[5], (D, 3, HH), D ** -0.5, 0.21875, ((0, 4), (2, 2))),
        "conv_kernel": normal_values(keys[6], (3, 3, HH), 3 ** -0.5, 3.5, ((2, 2),), jnp.float32),
        "conv_bias": normal_values(keys[7], (3, HH), 0.3, 1.8, ((1, 2),), jnp.float32),
        "out_weight": normal_values(keys[8], (HH, D), (max(HH // 64, 1)) ** -0.5, 1.75, ((0, 2), (1, 4))),
        "ln2_gain": jnp.clip(1.0 + 0.1 * jax.random.normal(keys[9], (D,), jnp.float32), 0.5, 1.5),
        "ln2_bias": normal_values(keys[10], (D,), 0.3, 1.8, (), jnp.float32),
        "up_weight": normal_values(keys[11], (D, FF), D ** -0.5, 0.21875, ((0, 4), (1, 2))),
        "down_weight": normal_values(keys[12], (FF, D), FF ** -0.5, 0.109375, ((0, 2), (1, 4))),
    }


@jax.custom_vjp
def low(v):
    return lax.optimization_barrier(v.astype(jnp.bfloat16)).astype(jnp.float32)

@jax.custom_vjp
def low_back(v):
    return v

def low_keep(v):
    return (low(v), None)

def low_pass(kept, grad):
    return (grad,)

def back_keep(v):
    return (v, None)

def back_low(kept, grad):
    return (low(grad),)
low.defvjp(low_keep, low_pass)
low_back.defvjp(back_keep, back_low)
EPSILON = 1e-05
SCALING = 0.125
MASKED = -1e+30
PRECISE = lax.Precision.HIGHEST

def layer_norm(row_data, norm_gain, shift_bias):
    centred = row_data - lax.optimization_barrier(jnp.mean(row_data, axis=-1, keepdims=True))
    recip = lax.rsqrt(lax.optimization_barrier(jnp.mean(centred * centred, axis=-1, keepdims=True)) + EPSILON)
    return centred * recip * norm_gain + shift_bias

def slot_forward(params, slot_tokens, slot_length):
    gain_one, bias_one, qkv_full, kernel, conv_shift, out_full, gain_two, bias_two, up_weights, down_weights = params
    positions = jnp.arange(S, dtype=jnp.int32)
    first_out = low(layer_norm(slot_tokens, gain_one, bias_one))
    pre_low = low_back(low(jnp.einsum('td,dcn->tcn', first_out, qkv_full, precision=PRECISE)))
    padded = jnp.pad(pre_low, ((2, 0), (0, 0), (0, 0)))
    conv_out = low(conv_shift + kernel[0] * padded[2:] + kernel[1] * padded[1:-1] + kernel[2] * padded[:-2])
    query_heads = conv_out[:, 0].reshape(S, H, HD)
    key_heads = conv_out[:, 1].reshape(S, H, HD)
    value_heads = conv_out[:, 2].reshape(S, H, HD)
    scores = low_back(jnp.einsum('qhd,khd->hqk', query_heads, key_heads, precision=PRECISE) * SCALING)
    allowed = (positions[None, :] <= positions[:, None]) & (positions[None, :] < slot_length)
    scores = jnp.where(allowed[None], scores, MASKED)
    row_max = lax.optimization_barrier(jnp.max(scores, axis=-1, keepdims=True))
    log_total = row_max + jnp.log(lax.optimization_barrier(jnp.sum(jnp.exp(scores - row_max), axis=-1, keepdims=True)))
    probs_low = low(jnp.exp(scores - log_total))
    attn_full = jnp.einsum('hqk,khd->qhd', probs_low, value_heads, precision=PRECISE).reshape(S, HH)
    attn_low = low_back(low(attn_full))
    middle = slot_tokens + low_back(jnp.dot(attn_low, out_full, precision=PRECISE))
    second_out = low(layer_norm(middle, gain_two, bias_two))
    up_full = low_back(jnp.dot(second_out, up_weights, precision=PRECISE))
    act_low = low(jnp.square(jnp.maximum(up_full, 0.0)))
    return middle + low_back(jnp.dot(act_low, down_weights, precision=PRECISE))

def reference(tokens, lengths, cotangent, ln1_gain, ln1_bias, qkv_weight, conv_kernel, conv_bias, out_weight, ln2_gain, ln2_bias, up_weight, down_weight):
    params = (ln1_gain, ln1_bias, qkv_weight.astype(jnp.float32), conv_kernel, conv_bias, out_weight.astype(jnp.float32), ln2_gain, ln2_bias, up_weight.astype(jnp.float32), down_weight.astype(jnp.float32))
    inputs = tokens.astype(jnp.float32)

    def forward(weights_all, inputs_all):
        checked = jax.checkpoint(slot_forward)
        return lax.map(lambda slot_pair: checked(weights_all, slot_pair[0], slot_pair[1]), (inputs_all, lengths))
    outputs, pullback = jax.vjp(forward, params, inputs)
    token_valid = (jnp.arange(S, dtype=jnp.int32)[None, :] < lengths[:, None]).astype(jnp.float32)
    grads, input_grad = pullback(cotangent.astype(jnp.float32) * token_valid[:, :, None])
    g_gain_one, g_bias_one, g_qkv, g_kernel, g_conv_shift, g_out, g_gain_two, g_bias_two, g_up, g_down = grads
    return (outputs.astype(jnp.bfloat16), input_grad, g_gain_one, g_bias_one, g_qkv, g_kernel, g_conv_shift, g_out, g_gain_two, g_bias_two, g_up, g_down)
```

```python
import jax
import jax.numpy as jnp
from jax import lax
from jax.sharding import PartitionSpec as P

HD = 64


EPSILON = 1e-05
SCALING = 0.125
MASKED = -1e30


def shifted(block, axis, distance):
    devices = range(lax.axis_size(axis))
    route = [(i - distance, i) for i in devices if i - distance in devices]
    return lax.ppermute(block, axis, route)


def layer_norm(row_data, norm_gain, shift_bias):
    centred = row_data - jnp.mean(row_data, axis=-1, keepdims=True)
    recip = lax.rsqrt(jnp.mean(centred * centred, axis=-1, keepdims=True) + EPSILON)
    normed = centred * recip
    return (normed * norm_gain + shift_bias, normed, recip)


def norm_back(grad_in, normed, recip, norm_gain):
    scaled = grad_in * norm_gain
    return recip * (
        scaled
        - jnp.mean(scaled, axis=-1, keepdims=True)
        - normed * jnp.mean(scaled * normed, axis=-1, keepdims=True)
    )


def tile_scores(query_part, key_part, query_pos, key_pos, lengths):
    scores = (
        jnp.einsum("mqhd,mkhd->mhqk", query_part, key_part, preferred_element_type=jnp.float32)
        * SCALING
    )
    allowed = (key_pos[None, None, :] <= query_pos[None, :, None]) & (
        key_pos[None, None, :] < lengths[:, None, None]
    )
    return jnp.where(allowed[:, None], scores, MASKED)


def tile_grads(
    query_part, key_part, value_part, grad_part, log_part, delta_part, query_pos, key_pos, lengths
):
    probs_full = jnp.exp(tile_scores(query_part, key_part, query_pos, key_pos, lengths) - log_part)
    prob_grad = jnp.einsum(
        "mqhd,mkhd->mhqk", grad_part, value_part, preferred_element_type=jnp.float32
    )
    score_grad = (probs_full * (prob_grad - delta_part)).astype(jnp.bfloat16)
    return (probs_full, prob_grad, score_grad)


def local(
    tokens,
    lengths,
    cotangent,
    ln1_gain,
    ln1_bias,
    qkv_weight,
    conv_kernel,
    conv_bias,
    out_weight,
    ln2_gain,
    ln2_bias,
    up_weight,
    down_weight,
):
    batches, block_rows, model_width = tokens.shape
    all_rows = batches * block_rows
    qkv_full, out_full, up_full_w, down_full_w = (
        lax.all_gather(qkv_weight, "fsdp", axis=0, tiled=True),
        lax.all_gather(out_weight, "fsdp", axis=1, tiled=True),
        lax.all_gather(up_weight, "fsdp", axis=0, tiled=True),
        lax.all_gather(down_weight, "fsdp", axis=1, tiled=True),
    )
    local_width = qkv_full.shape[2]
    local_heads = local_width // HD
    ctx_count = lax.axis_size("ctx")
    slot_span = block_rows * ctx_count
    group_blocks = 4
    key_span = block_rows * group_blocks
    ctx_index = lax.axis_index("ctx")
    positions = ctx_index * block_rows + jnp.arange(block_rows, dtype=jnp.int32)
    span_iota = jnp.arange(key_span, dtype=jnp.int32)
    block_count = (ctx_index * block_rows + block_rows + key_span - 1) // key_span
    token_valid = positions[None, :] < lengths[:, None]

    def span_slice(array_data, block, axis_pos):
        return lax.dynamic_slice_in_dim(array_data, block * key_span, key_span, axis_pos)

    inputs = tokens.astype(jnp.float32).reshape(all_rows, model_width)
    first_out, first_hat, first_recip = layer_norm(inputs, ln1_gain, ln1_bias)
    first_low = first_out.astype(jnp.bfloat16)
    pre_low = jnp.einsum(
        "td,dcn->tcn", first_low, qkv_full, preferred_element_type=jnp.float32
    ).astype(jnp.bfloat16)
    pre_low = pre_low.reshape(batches, block_rows, 3, local_width)
    earlier = shifted(pre_low[:, block_rows - 2 :], "ctx", 1)
    extended = jnp.concatenate([earlier, pre_low], axis=1).astype(jnp.float32)
    conv_out = (
        conv_bias
        + conv_kernel[0] * extended[:, 2:]
        + conv_kernel[1] * extended[:, 1:-1]
        + conv_kernel[2] * extended[:, :-2]
    ).astype(jnp.bfloat16)
    query_heads = conv_out[:, :, 0].reshape(batches, block_rows, local_heads, HD)
    own_pairs = conv_out[:, :, 1:]
    whole_pairs = lax.all_gather(own_pairs, "ctx", axis=1, tiled=True)
    key_heads = whole_pairs[:, :, 0].reshape(batches, slot_span, local_heads, HD)
    value_heads = whole_pairs[:, :, 1].reshape(batches, slot_span, local_heads, HD)

    def stat_step(block, carry):
        row_max, total = carry
        key_pos = block * key_span + span_iota
        scores = tile_scores(
            query_heads, span_slice(key_heads, block, 1), positions, key_pos, lengths
        )
        new_max = jnp.maximum(row_max, jnp.max(scores, axis=-1, keepdims=True))
        total = total * jnp.exp(row_max - new_max) + jnp.sum(
            jnp.exp(scores - new_max), axis=-1, keepdims=True
        )
        return (new_max, total)

    stat_shape = (batches, local_heads, block_rows, 1)
    row_max, total = lax.fori_loop(
        0,
        block_count,
        stat_step,
        (jnp.full(stat_shape, MASKED, jnp.float32), jnp.zeros(stat_shape, jnp.float32)),
    )
    log_total = row_max + jnp.log(total)

    def value_step(block, accum):
        key_pos = block * key_span + span_iota
        scores = tile_scores(
            query_heads, span_slice(key_heads, block, 1), positions, key_pos, lengths
        )
        probs_low = jnp.exp(scores - log_total).astype(jnp.bfloat16)
        return accum + jnp.einsum(
            "mhqk,mkhd->mqhd",
            probs_low,
            span_slice(value_heads, block, 1),
            preferred_element_type=jnp.float32,
        )

    attn_acc = lax.fori_loop(
        0, block_count, value_step, jnp.zeros((batches, block_rows, local_heads, HD), jnp.float32)
    )
    attn_low = attn_acc.reshape(all_rows, local_width).astype(jnp.bfloat16)
    attn_out = lax.psum(jnp.dot(attn_low, out_full, preferred_element_type=jnp.float32), "tp")
    middle = inputs + attn_out
    second_out, second_hat, second_recip = layer_norm(middle, ln2_gain, ln2_bias)
    second_low = second_out.astype(jnp.bfloat16)
    up_full = jnp.dot(second_low, up_full_w, preferred_element_type=jnp.float32)
    rectified = jnp.maximum(up_full, 0.0)
    act_low = (rectified * rectified).astype(jnp.bfloat16)
    ffn_out = lax.psum(jnp.dot(act_low, down_full_w, preferred_element_type=jnp.float32), "tp")
    result = (middle + ffn_out).reshape(batches, block_rows, model_width).astype(jnp.bfloat16)
    grad_out = (
        cotangent.astype(jnp.float32) * token_valid[:, :, None].astype(jnp.float32)
    ).reshape(all_rows, model_width)
    grad_low = grad_out.astype(jnp.bfloat16)
    down_wgrad = jnp.einsum("tf,td->fd", act_low, grad_low, preferred_element_type=jnp.float32)
    act_grad = jnp.einsum("td,fd->tf", grad_low, down_full_w, preferred_element_type=jnp.float32)
    up_grad_low = (act_grad * 2.0 * rectified).astype(jnp.bfloat16)
    up_wgrad = jnp.einsum("td,tf->df", second_low, up_grad_low, preferred_element_type=jnp.float32)
    second_grad = lax.psum(
        jnp.einsum("tf,df->td", up_grad_low, up_full_w, preferred_element_type=jnp.float32), "tp"
    )
    gain_two_grad = jnp.sum(second_grad * second_hat, axis=0)
    bias_two_grad = jnp.sum(second_grad, axis=0)
    middle_grad = grad_out + norm_back(second_grad, second_hat, second_recip, ln2_gain)
    middle_low = middle_grad.astype(jnp.bfloat16)
    out_wgrad = jnp.einsum("tn,td->nd", attn_low, middle_low, preferred_element_type=jnp.float32)
    attn_flat = jnp.einsum(
        "td,nd->tn", middle_low, out_full, preferred_element_type=jnp.float32
    ).astype(jnp.bfloat16)
    attn_grad = attn_flat.reshape(batches, block_rows, local_heads, HD)

    def delta_step(block, accum):
        key_pos = block * key_span + span_iota
        probs_full = jnp.exp(
            tile_scores(query_heads, span_slice(key_heads, block, 1), positions, key_pos, lengths)
            - log_total
        )
        prob_grad = jnp.einsum(
            "mqhd,mkhd->mhqk",
            attn_grad,
            span_slice(value_heads, block, 1),
            preferred_element_type=jnp.float32,
        )
        return accum + jnp.sum(probs_full * prob_grad, axis=-1, keepdims=True)

    delta = lax.fori_loop(0, block_count, delta_step, jnp.zeros(stat_shape, jnp.float32))
    query_zero = jnp.zeros((batches, block_rows, local_heads, HD), jnp.float32)

    def back_step(block, carry):
        accum, buffer = carry
        key_pos = block * key_span + span_iota
        key_part = span_slice(key_heads, block, 1)
        probs_full, prob_grad, score_grad = tile_grads(
            query_heads,
            key_part,
            span_slice(value_heads, block, 1),
            attn_grad,
            log_total,
            delta,
            positions,
            key_pos,
            lengths,
        )
        probs_again = probs_full.astype(jnp.bfloat16)
        accum = (
            accum
            + jnp.einsum(
                "mhqk,mkhd->mqhd", score_grad, key_part, preferred_element_type=jnp.float32
            )
            * SCALING
        )
        key_term = (
            jnp.einsum(
                "mhqk,mqhd->mkhd", score_grad, query_heads, preferred_element_type=jnp.float32
            )
            * SCALING
        )
        value_term = jnp.einsum(
            "mhqk,mqhd->mkhd", probs_again, attn_grad, preferred_element_type=jnp.float32
        )
        stacked = jnp.stack(
            [
                key_term.reshape(batches, key_span, local_width),
                value_term.reshape(batches, key_span, local_width),
            ],
            axis=2,
        )
        buffer = lax.dynamic_update_slice_in_dim(buffer, stacked, block * key_span, 1)
        return (accum, buffer)

    buffer_zero = jnp.zeros((batches, slot_span, 2, local_width), jnp.float32)
    query_grad, pair_terms = lax.fori_loop(0, block_count, back_step, (query_zero, buffer_zero))
    pair_grad = lax.psum_scatter(pair_terms, "ctx", scatter_dimension=1, tiled=True)
    mixed_grad = jnp.concatenate(
        [query_grad.reshape(batches, block_rows, 1, local_width), pair_grad], axis=2
    )
    later = shifted(mixed_grad[:, :2], "ctx", -1)
    ahead = jnp.concatenate([mixed_grad, later], axis=1)
    pre_grad = (
        conv_kernel[0] * ahead[:, :block_rows]
        + conv_kernel[1] * ahead[:, 1 : block_rows + 1]
        + conv_kernel[2] * ahead[:, 2:]
    ).astype(jnp.bfloat16)
    kernel_grad = jnp.stack(
        [
            jnp.sum(extended[:, 2 - offset : 2 - offset + block_rows] * mixed_grad, axis=(0, 1))
            for offset in range(3)
        ]
    )
    shift_grad = jnp.sum(mixed_grad, axis=(0, 1))
    pre_grad = pre_grad.reshape(all_rows, 3, local_width)
    qkv_wgrad = jnp.einsum("td,tcn->dcn", first_low, pre_grad, preferred_element_type=jnp.float32)
    first_grad = lax.psum(
        jnp.einsum("tcn,dcn->td", pre_grad, qkv_full, preferred_element_type=jnp.float32), "tp"
    )
    gain_one_grad = jnp.sum(first_grad * first_hat, axis=0)
    bias_one_grad = jnp.sum(first_grad, axis=0)
    input_grad = middle_grad + norm_back(first_grad, first_hat, first_recip, ln1_gain)
    input_grad = input_grad.reshape(batches, block_rows, model_width)
    def owned(term, axis_pos):
        part = lax.psum_scatter(
            term.astype(jnp.bfloat16), "fsdp", scatter_dimension=axis_pos, tiled=True
        )
        return lax.psum(part, "ctx").astype(jnp.float32)

    qkv_share = owned(qkv_wgrad, 0)
    out_share = owned(out_wgrad, 1)
    up_share = owned(up_wgrad, 0)
    down_share = owned(down_wgrad, 1)
    small_sums = lax.psum(
        (
            gain_one_grad,
            bias_one_grad,
            kernel_grad,
            shift_grad,
            gain_two_grad,
            bias_two_grad,
        ),
        ("fsdp", "ctx"),
    )
    return (
        result,
        input_grad,
        small_sums[0],
        small_sums[1],
        qkv_share,
        small_sums[2],
        small_sums[3],
        out_share,
        small_sums[4],
        small_sums[5],
        up_share,
        down_share,
    )


def solution(mesh):
    placed = (
        P("fsdp", "ctx", None),
        P("fsdp"),
        P("fsdp", "ctx", None),
        P(),
        P(),
        P("fsdp", None, "tp"),
        P(None, None, "tp"),
        P(None, "tp"),
        P("tp", "fsdp"),
        P(),
        P(),
        P("fsdp", "tp"),
        P("tp", "fsdp"),
    )
    return jax.shard_map(
        local,
        mesh=mesh,
        in_specs=placed,
        out_specs=(
            P("fsdp", "ctx", None),
            P("fsdp", "ctx", None),
            P(),
            P(),
            P("fsdp", None, "tp"),
            P(None, None, "tp"),
            P(None, "tp"),
            P("tp", "fsdp"),
            P(),
            P(),
            P("fsdp", "tp"),
            P("tp", "fsdp"),
        ),
        check_vma=False,
    )
```
